256 devices in a mesh: trial: 2 (over core), qa: 16 (over y, x), qb: 8 (over z).
Axes of the slice: x: 4, y: 4, z: 8, core: 2. Of those that a mesh axis runs over, the one named last changes fastest.
Arguments:
- wave_parts: float32 [4, 512, 128, 128], P('trial', ('qa', 'qb')), parts along dimension 0, may hold values from -6 to 6
- level_table: float32 [1024, 128, 128], P(('trial', 'qa', 'qb')), parts along dimension 0, may hold values from -2 to 2
- diagonal_angles: float32 [6, 128], P('trial'), parts along dimension 0, may hold values from 0.3 to 1.2
- turn_angles: float32 [6, 4], P('trial'), parts along dimension 0, may hold values from 0.3 to 1.2
Outputs:
- final_parts: float32 [4, 512, 128, 128], P('trial', ('qa', 'qb')), parts along dimension 0
The draws below stay inside these ranges and needn't reach their ends.
There are 2 independent parts, one for each index of `trial`. The reference program is written for one: setup_inputs(seed, part) draws one part's arguments, and reference() takes and returns one part's arrays. A program takes and returns all parts, laid end to end along the dimension named above; each array names one. Nothing has to cross between parts.
All inputs are finite; a program needn't handle non-finite values.
Results may differ from the reference program's by a relative error of at most 0.0003.
Values sent between devices are 32-bit elements.
No kernel may reach another device: no remote copies, remote signals or barrier semaphores. Data moves between devices by JAX's collectives and lax.ppermute only.
A program may use at most 64 MiB of HBM per device.

```python
import jax
import jax.numpy as jnp
from jax import lax

BLOCKS_DEV = 4
ROWS = 128
LANES = 128
BLOCKS = 512
LAYERS = 3
N_QA = 16
N_QB = 8


def block_scale(own_key, dims, pieces, smallest, high):
    def one(position, blocks):
        heights = jax.random.uniform(jax.random.fold_in(jax.random.fold_in(own_key, 6), position), (blocks,), jnp.float32, smallest / len(pieces), high / len(pieces))
        return jnp.repeat(jnp.exp(heights), dims[position] // blocks).reshape((-1,) + (1,) * (len(dims) - position - 1))

    factor_of = one(*pieces[0])
    for cut in pieces[1:]:
        factor_of = factor_of * one(*cut)
    return factor_of


def scatter_about(rng, dims, spread, most, cuts=(), kind=jnp.bfloat16):
    values = spread * jax.random.normal(rng, dims, jnp.float32)
    if cuts:
        values = values * block_scale(rng, dims, cuts, -0.22, 0.18)
    return jnp.clip(values, -most, most).astype(kind)


def setup_inputs(seed: int = 0, part: int = 0) -> dict:
    key_of = jax.random.split(jax.random.key(seed), 5)
    own_keys = jax.random.split(jax.random.fold_in(key_of[4], part), 5)
    wave_parts = scatter_about(own_keys[0], (2, BLOCKS, ROWS, LANES), 1.0, 6.0, ((1, 128),), jnp.float32)
    level_table = jnp.clip(jax.random.uniform(own_keys[1], (BLOCKS, ROWS, LANES), jnp.float32, -2.0, 2.0) * block_scale(own_keys[1], (BLOCKS, ROWS, LANES), ((0, 128),), -0.4, 0.0), -2.0, 2.0)
    diagonal_angles = jnp.clip(jax.random.uniform(own_keys[2], (LAYERS, LANES), jnp.float32, 0.3, 1.2), 0.3, 1.2)
    turn_angles = jnp.clip(jax.random.uniform(own_keys[3], (LAYERS, 4), jnp.float32, 0.3, 1.2), 0.3, 1.2)
    return dict(wave_parts=wave_parts, level_table=level_table, diagonal_angles=diagonal_angles, turn_angles=turn_angles)


def count_bits(values, count):
    places = jnp.arange(count.bit_length() - 1, dtype=jnp.int32)
    return jnp.sum((values[..., None] >> places) & 1, axis=-1)


def rotation_table(count, angle):
    rank = jnp.arange(count, dtype=jnp.int32)
    apart = count_bits(rank[:, None] ^ rank[None, :], count)
    bits = count.bit_length() - 1
    size = jnp.cos(angle) ** (bits - apart).astype(jnp.float32) * jnp.sin(angle) ** apart.astype(jnp.float32)
    real_sign = jnp.where(apart % 4 == 0, 1.0, jnp.where(apart % 4 == 2, -1.0, 0.0)).astype(jnp.float32)
    imag_sign = jnp.where(apart % 4 == 1, -1.0, jnp.where(apart % 4 == 3, 1.0, 0.0)).astype(jnp.float32)
    return size * real_sign, size * imag_sign


def mix_dim(values, dim, angle):
    real_part, imag_part = rotation_table(values.shape[dim], angle)
    def times(table):
        moved = jnp.tensordot(values, table, axes=([dim], [0]), precision=lax.Precision.HIGHEST)
        return jnp.moveaxis(moved, -1, dim)
    by_real = times(real_part)
    by_imag = times(imag_part)
    return jnp.stack([by_real[0] - by_imag[1], by_real[1] + by_imag[0]])


def phase_step(values, levels, angle):
    turn = angle * levels
    return jnp.stack([values[0] * jnp.cos(turn) + values[1] * jnp.sin(turn), values[1] * jnp.cos(turn) - values[0] * jnp.sin(turn)])


def reference(wave_parts, level_table, diagonal_angles, turn_angles):
    values = wave_parts
    for layer in range(LAYERS):
        values = phase_step(values, level_table, diagonal_angles[layer])
        values = mix_dim(values, 3, turn_angles[layer, 0])
        values = mix_dim(values, 2, turn_angles[layer, 1])
        parts = values.reshape(2, N_QA, N_QB, BLOCKS_DEV, ROWS, LANES)
        parts = mix_dim(parts, 1, turn_angles[layer, 2])
        parts = mix_dim(parts, 2, turn_angles[layer, 3])
        parts = mix_dim(parts, 3, turn_angles[layer, 2])
        values = parts.reshape(values.shape)
    return values
```

```python
import jax
import jax.numpy as jnp
from jax import lax
from jax.sharding import PartitionSpec as P

LAYERS = 3
HIGH = lax.Precision.HIGHEST


def count_bits(values):
    places = jnp.arange(10, dtype=jnp.int32)
    return jnp.sum(values[..., None] >> places & 1, axis=-1)


def rotation(count, angle):
    rank = jnp.arange(count, dtype=jnp.int32)
    to, of = rank[:, None], rank[None, :]
    apart = count_bits(to ^ of)
    bits = count.bit_length() - 1
    size = jnp.cos(angle) ** (bits - apart).astype(jnp.float32) * jnp.sin(angle) ** apart.astype(
        jnp.float32
    )
    return jnp.where(count_bits(to & ~of) % 2 == 0, size, -size)


def quarter_turns(real, imag, turns):
    odd = turns % 2 == 1
    new_real = jnp.where(odd, -imag, real)
    new_imag = jnp.where(odd, real, imag)
    sign = jnp.where(turns % 4 >= 2, -1.0, 1.0).astype(jnp.float32)
    return new_real * sign, new_imag * sign


def phase(real, imag, turn):
    cos, sin = jnp.cos(turn), jnp.sin(turn)
    return real * cos + imag * sin, imag * cos - real * sin


def exchange(values):
    return lax.all_to_all(values, ("qa", "qb"), split_axis=0, concat_axis=0, tiled=True)


def shards(wave_parts, level_table, diagonal_angles, turn_angles):
    n_qa, n_qb = lax.axis_size("qa"), lax.axis_size("qb")
    place = lax.axis_index("qa") * n_qb + lax.axis_index("qb")
    n_q = n_qa * n_qb
    blocks, rows, lanes = level_table.shape
    lane_mix = [rotation(lanes, turn_angles[i, 0]) for i in range(LAYERS)]
    row_mix = [rotation(rows, turn_angles[i, 1]) for i in range(LAYERS)]
    block_mix = [rotation(blocks, turn_angles[i, 2]) for i in range(LAYERS)]
    q_mix = [
        jnp.kron(rotation(n_qa, turn_angles[i, 2]), rotation(n_qb, turn_angles[i, 3]))
        for i in range(LAYERS)
    ]

    turns = (
        count_bits(place)
        + count_bits(jnp.arange(blocks))[:, None, None]
        + count_bits(jnp.arange(rows))[None, :, None]
        + count_bits(jnp.arange(lanes))[None, None, :]
    )

    real, imag = quarter_turns(wave_parts[0], wave_parts[1], -turns % 4)
    real, imag = phase(real, imag, diagonal_angles[0] * level_table)
    values = jnp.stack([real, imag])
    values = jnp.einsum("cbrl,kl->cbrk", values, lane_mix[0], precision=HIGH)
    values = jnp.einsum("cbrk,ab->cark", values, block_mix[0], precision=HIGH)
    values = jnp.einsum("cark,sr->scak", values, row_mix[0], precision=HIGH)
    sent = jnp.concatenate(
        [
            values.reshape(rows, 2 * blocks, lanes),
            jnp.moveaxis(level_table, 1, 0),
            jnp.moveaxis(level_table, 2, 0),
        ],
        axis=1,
    )
    got = exchange(sent)

    values = got[:, : 2 * blocks].reshape(n_q, 2, blocks, lanes)
    by_row, by_lane = got[:, 2 * blocks : 3 * blocks], got[:, 3 * blocks :]
    values = jnp.einsum("pq,qcbl->pcbl", q_mix[0], values, precision=HIGH)
    real, imag = phase(values[:, 0], values[:, 1], diagonal_angles[1] * by_row)
    values = jnp.stack([real, imag], axis=1)
    values = jnp.einsum("pq,qcbl->pcbl", q_mix[1], values, precision=HIGH)
    values = jnp.einsum("ab,qcbl->qcal", block_mix[1], values, precision=HIGH)
    values = jnp.einsum("kl,qcal->kcaq", lane_mix[1], values, precision=HIGH)
    values = exchange(values.reshape(lanes, 2 * blocks, n_q)).reshape(rows, 2, blocks, n_q)

    values = jnp.einsum("sr,rcbq->scbq", row_mix[1], values, precision=HIGH)
    own_angle = lax.dynamic_index_in_dim(diagonal_angles[2], place, 0, keepdims=False)
    real, imag = phase(values[:, 0], values[:, 1], own_angle * jnp.transpose(by_lane, (2, 1, 0)))
    values = jnp.stack([real, imag], axis=1)
    values = jnp.einsum("sr,rcbq->scbq", row_mix[2], values, precision=HIGH)
    values = jnp.einsum("ab,rcbq->rcaq", block_mix[2], values, precision=HIGH)
    values = jnp.einsum("pq,rcaq->pcar", q_mix[2], values, precision=HIGH)
    values = exchange(values.reshape(n_q, 2 * blocks, rows)).reshape(lanes, 2, blocks, rows)

    values = jnp.einsum("kl,lcbr->cbrk", lane_mix[2], values, precision=HIGH)
    real, imag = quarter_turns(values[0], values[1], turns)
    return jnp.stack([real, imag])


def solution(mesh):
    placed = (
        P("trial", ("qa", "qb"), None, None),
        P(("trial", "qa", "qb"), None, None),
        P("trial", None),
        P("trial", None),
    )
    return jax.shard_map(
        shards,
        mesh=mesh,
        in_specs=placed,
        out_specs=P("trial", ("qa", "qb"), None, None),
        check_vma=False,
    )
```

```python
import jax
import jax.numpy as jnp
from jax import lax
from jax.experimental import pallas as pl
from jax.experimental.pallas import tpu as pltpu
from jax.sharding import PartitionSpec as P

SIDE = 128
BITS = 7
BLOCKS = 4
PARTS = 2
TILE = PARTS * BLOCKS
TABLES = 2 * BLOCKS
QB_BITS = 3


def sin_cos(angle, turns=None):
    near = jnp.floor(angle * 0.6366197723675814 + 0.5)
    left = ((angle - near * 1.5703125) - near * 4.837512969970703e-4) - near * 7.549789954891882e-8
    quarter = near.astype(jnp.int32)
    if turns is not None:
        quarter = quarter + turns
    sq = left * left
    sine = left + left * sq * (-1.6666654611e-1 + sq * (8.3321608736e-3 - sq * 1.9515295891e-4))
    cosine = (1.0 - 0.5 * sq) + sq * sq * (
        4.166664568298827e-2 + sq * (-1.388731625493765e-3 + sq * 2.443315711809948e-5)
    )
    odd = (quarter & 1) == 1
    new_sine = jnp.where(odd, cosine, sine)
    new_cosine = jnp.where(odd, sine, cosine)
    new_sine = jnp.where((quarter & 2) != 0, -new_sine, new_sine)
    new_cosine = jnp.where(((quarter + 1) & 2) != 0, -new_cosine, new_cosine)
    return new_sine, new_cosine


def pair_of(angles, layer, group):
    return sin_cos(jnp.full((1, SIDE), angles[layer, group], jnp.float32))


def butterfly(values, pairs):
    values = list(values)
    for bit, (sine, cosine) in enumerate(pairs):
        step = 1 << bit
        for low in range(len(values)):
            if not low & step:
                u, v = values[low], values[low + step]
                values[low] = cosine * u + sine * v
                values[low + step] = cosine * v - sine * u
    return values


def mix_tiles(load, store, pairs):
    for high in range(0, SIDE, 8):
        for i, value in enumerate(butterfly([load(high + i) for i in range(8)], pairs[:3])):
            store(high + i, value, 0)
    for low in range(8):
        order = range(low, SIDE, 8)
        for i, value in zip(order, butterfly([store(i, None, 0) for i in order], pairs[3:])):
            store(i, value, 1)


def weights(pairs):
    lane = lax.broadcasted_iota(jnp.int32, (8, SIDE), 1)
    sub = lax.broadcasted_iota(jnp.int32, (8, SIDE), 0)

    def factor(bit, of):
        to = (lane >> bit) & 1
        sine, cosine = pairs[bit]
        return jnp.where(of == to, cosine, jnp.where(to == 1, -sine, sine))

    matrix = factor(0, sub & 1) * factor(1, (sub >> 1) & 1) * factor(2, (sub >> 2) & 1)
    for bit in range(3, BITS):
        ends = [factor(bit, jnp.full((8, SIDE), of, jnp.int32)) for of in (0, 1)]
        pieces = matrix.shape[0] // 8
        matrix = jnp.concatenate(
            [matrix[8 * i : 8 * i + 8] * end for end in ends for i in range(pieces)], axis=0
        )
    high = matrix.astype(jnp.bfloat16)
    low = (matrix - high.astype(jnp.float32)).astype(jnp.bfloat16)
    both = jnp.concatenate([high, low], axis=1)
    return jnp.concatenate([both, both], axis=0)


def mix_lanes(values, both):
    high = values.astype(jnp.bfloat16)
    low = (values - high.astype(jnp.float32)).astype(jnp.bfloat16)
    out = jnp.dot(
        jnp.concatenate([high, low], axis=1), both, preferred_element_type=jnp.float32
    )
    return out[:, :SIDE] + out[:, SIDE:]


def bit_counts(place):
    row = lax.broadcasted_iota(jnp.int32, (SIDE, SIDE), 0)
    lane = lax.broadcasted_iota(jnp.int32, (SIDE, SIDE), 1)
    total = jnp.full((SIDE, SIDE), place, jnp.int32)
    count = jnp.zeros((SIDE, SIDE), jnp.int32)
    for bit in range(BITS):
        count = count + ((row >> bit) & 1) + ((lane >> bit) & 1) + ((total >> bit) & 1)
    return count


def every(step, first, count=SIDE):
    return pl.ds(first, count, stride=step)


def turned(real, imag, sine, cosine):
    return real * cosine + imag * sine, imag * cosine - real * sine


def mix_blocks(parts, pair):
    return [butterfly(part, [pair] * 2) for part in parts]


def in_buffer(buffer, out=None, step=TILE):
    def store(index, value, last):
        if value is None:
            return buffer[TILE * index : TILE * index + TILE, :]
        if last and out is not None:
            out[step * index : step * index + TILE, :] = value
        else:
            buffer[TILE * index : TILE * index + TILE, :] = value

    return store


def first_kernel(angles, place, diagonal, wave, levels, out, buffer):
    group = [pair_of(angles, 0, g) for g in range(4)]
    lane_mix = weights([group[0]] * BITS)
    count = bit_counts(place[0, 0])
    speed = diagonal[0:1, :]
    real, imag = [], []
    for b in range(BLOCKS):
        level = levels[b]
        sine, cosine = sin_cos(level * speed, count + b.bit_count())
        r, i = turned(wave[0, b], wave[1, b], sine, cosine)
        real.append(r)
        imag.append(i)
        out[every(TILE + TABLES, TILE + b), :] = level
        out[every(TILE + TABLES, TILE + BLOCKS + b), :] = level.T
    for p, part in enumerate(mix_blocks((real, imag), group[2])):
        for b in range(BLOCKS):
            buffer[every(TILE, p * BLOCKS + b), :] = mix_lanes(part[b], lane_mix)
    store = in_buffer(buffer, out, TILE + TABLES)
    mix_tiles(lambda i: store(i, None, 0), store, [group[1]] * BITS)


def second_kernel(angles, diagonal, got, out, turned_levels, buffer):
    q_pairs = [pair_of(angles, 0, 3)] * QB_BITS + [pair_of(angles, 0, 2)] * (BITS - QB_BITS)
    step = TILE + TABLES
    store = in_buffer(buffer)
    mix_tiles(lambda i: got[step * i : step * i + TILE, :], store, q_pairs)
    group = [pair_of(angles, 1, g) for g in range(4)]
    lane_mix = weights([group[0]] * BITS)
    q_mix = weights([group[3]] * QB_BITS + [group[2]] * (BITS - QB_BITS))
    speed = diagonal[1:2, :]
    real, imag = [], []
    for b in range(BLOCKS):
        sine, cosine = sin_cos(got[every(step, TILE + b), :] * speed)
        r, i = turned(
            buffer[every(TILE, b), :], buffer[every(TILE, BLOCKS + b), :], sine, cosine
        )
        real.append(r)
        imag.append(i)
        turned_levels[b] = got[every(step, TILE + BLOCKS + b), :].T
    for p, part in enumerate(mix_blocks((real, imag), group[2])):
        for b in range(BLOCKS):
            out[every(TILE, p * BLOCKS + b), :] = mix_lanes(mix_lanes(part[b], lane_mix).T, q_mix)


def third_kernel(angles, place, diagonal, got, turned_levels, out, buffer):
    store = in_buffer(buffer)
    mix_tiles(
        lambda i: got[TILE * i : TILE * i + TILE, :], store, [pair_of(angles, 1, 1)] * BITS
    )
    group = [pair_of(angles, 2, g) for g in range(4)]
    q_mix = weights([group[3]] * QB_BITS + [group[2]] * (BITS - QB_BITS))
    row_mix = weights([group[1]] * BITS)
    lane = lax.broadcasted_iota(jnp.int32, (1, SIDE), 1)
    speed = jnp.sum(jnp.where(lane == place[0, 0], diagonal[2:3, :], 0.0), axis=1, keepdims=True)
    real, imag = [], []
    for b in range(BLOCKS):
        sine, cosine = sin_cos(turned_levels[b] * speed)
        r, i = turned(
            buffer[every(TILE, b), :], buffer[every(TILE, BLOCKS + b), :], sine, cosine
        )
        real.append(r)
        imag.append(i)
    for p, part in enumerate(mix_blocks((real, imag), group[2])):
        for b in range(BLOCKS):
            out[every(TILE, p * BLOCKS + b), :] = mix_lanes(mix_lanes(part[b], q_mix).T, row_mix)


def last_kernel(angles, place, got, out, buffer):
    store = in_buffer(buffer)
    mix_tiles(
        lambda i: got[TILE * i : TILE * i + TILE, :], store, [pair_of(angles, 2, 0)] * BITS
    )
    count = bit_counts(place[0, 0])
    for b in range(BLOCKS):
        real, imag = (buffer[every(TILE, p * BLOCKS + b), :].T for p in range(PARTS))
        turns = count + b.bit_count()
        odd = (turns & 1) == 1
        new_real, new_imag = jnp.where(odd, -imag, real), jnp.where(odd, real, imag)
        back = (turns & 2) != 0
        out[0, b] = jnp.where(back, -new_real, new_real)
        out[1, b] = jnp.where(back, -new_imag, new_imag)


def call(kernel, name, operands, outs, interpret=False):
    small = pl.BlockSpec(memory_space=pltpu.SMEM)
    big = pl.BlockSpec(memory_space=pltpu.VMEM)
    specs = [small if o.size <= 16 else big for o in operands]
    shapes = [jax.ShapeDtypeStruct(s, jnp.float32) for s in outs]
    return pl.pallas_call(
        kernel,
        name=name,
        in_specs=specs,
        out_specs=[big] * len(outs),
        out_shape=shapes,
        scratch_shapes=[pltpu.VMEM((SIDE * TILE, SIDE), jnp.float32)],
        compiler_params=pltpu.CompilerParams(vmem_limit_bytes=32 * 1024 * 1024),
        interpret=interpret,
    )(*operands)


def exchange(values):
    shape = values.shape
    moved = lax.all_to_all(
        values.reshape(SIDE, -1, SIDE), ("qa", "qb"), split_axis=0, concat_axis=0, tiled=True
    )
    return moved.reshape(shape)


def stages(interpret=False):
    tile = (SIDE * TILE, SIDE)

    def first(angles, place, diagonal, wave, levels):
        shape = (SIDE * (TILE + TABLES), SIDE)
        return call(first_kernel, "first", (angles, place, diagonal, wave, levels), [shape], interpret)[0]

    def second(angles, diagonal, got):
        return call(
            second_kernel, "second", (angles, diagonal, got), [tile, (BLOCKS, SIDE, SIDE)], interpret
        )

    def third(angles, place, diagonal, got, levels):
        return call(third_kernel, "third", (angles, place, diagonal, got, levels), [tile], interpret)[0]

    def last(angles, place, got):
        return call(
            last_kernel, "last", (angles, place, got), [(PARTS, BLOCKS, SIDE, SIDE)], interpret
        )[0]

    return first, second, third, last


def shards(wave_parts, level_table, diagonal_angles, turn_angles):
    place = lax.axis_index("qa") * lax.axis_size("qb") + lax.axis_index("qb")
    place = jnp.full((1, 1), place, jnp.int32)
    first, second, third, last = stages()
    got = exchange(first(turn_angles, place, diagonal_angles, wave_parts, level_table))
    values, levels = second(turn_angles, diagonal_angles, got)
    values = third(turn_angles, place, diagonal_angles, exchange(values), levels)
    return last(turn_angles, place, exchange(values))


def solution(mesh):
    placed = (
        P("trial", ("qa", "qb"), None, None),
        P(("trial", "qa", "qb"), None, None),
        P("trial", None),
        P("trial", None),
    )
    return jax.shard_map(
        shards,
        mesh=mesh,
        in_specs=placed,
        out_specs=P("trial", ("qa", "qb"), None, None),
        check_vma=False,
    )
```

```python
import jax
import jax.numpy as jnp
from jax import lax
from jax.experimental import pallas as pl
from jax.experimental.pallas import tpu as pltpu
from jax.sharding import PartitionSpec as P

SIDE = 128
BITS = 7
BLOCKS = 4
PARTS = 2
TILE = PARTS * BLOCKS
WIDE = TILE + BLOCKS
QB_BITS = 3


def sin_cos(angle, turns=None):
    near = jnp.floor(angle * 0.6366197723675814 + 0.5)
    left = ((angle - near * 1.5703125) - near * 4.837512969970703e-4) - near * 7.549789954891882e-8
    quarter = near.astype(jnp.int32)
    if turns is not None:
        quarter = quarter + turns
    sq = left * left
    sine = left + left * sq * (-1.6666654611e-1 + sq * (8.3321608736e-3 - sq * 1.9515295891e-4))
    cosine = (1.0 - 0.5 * sq) + sq * sq * (
        4.166664568298827e-2 + sq * (-1.388731625493765e-3 + sq * 2.443315711809948e-5)
    )
    odd = (quarter & 1) == 1
    new_sine = jnp.where(odd, cosine, sine)
    new_cosine = jnp.where(odd, sine, cosine)
    new_sine = jnp.where((quarter & 2) != 0, -new_sine, new_sine)
    new_cosine = jnp.where(((quarter + 1) & 2) != 0, -new_cosine, new_cosine)
    return new_sine, new_cosine


def pair_of(angles, layer, group):
    return sin_cos(jnp.broadcast_to(angles[layer : layer + 1, group : group + 1], (1, SIDE)))


def butterfly(values, pairs):
    values = list(values)
    for bit, (sine, cosine) in enumerate(pairs):
        step = 1 << bit
        for low in range(len(values)):
            if not low & step:
                u, v = values[low], values[low + step]
                values[low] = cosine * u + sine * v
                values[low + step] = cosine * v - sine * u
    return values


def mix_tiles(load, store, pairs):
    for high in range(0, SIDE, 8):
        for i, value in enumerate(butterfly([load(high + i) for i in range(8)], pairs[:3])):
            store(high + i, value, 0)
    for low in range(8):
        order = range(low, SIDE, 8)
        for i, value in zip(order, butterfly([store(i, None, 0) for i in order], pairs[3:])):
            store(i, value, 1)


def weights(pairs):
    lane = lax.broadcasted_iota(jnp.int32, (8, SIDE), 1)
    sub = lax.broadcasted_iota(jnp.int32, (8, SIDE), 0)

    def factor(bit, of):
        to = (lane >> bit) & 1
        sine, cosine = pairs[bit]
        return jnp.where(of == to, cosine, jnp.where(to == 1, -sine, sine))

    matrix = factor(0, sub & 1) * factor(1, (sub >> 1) & 1) * factor(2, (sub >> 2) & 1)
    for bit in range(3, BITS):
        ends = [factor(bit, jnp.full((8, SIDE), of, jnp.int32)) for of in (0, 1)]
        pieces = matrix.shape[0] // 8
        matrix = jnp.concatenate(
            [matrix[8 * i : 8 * i + 8] * end for end in ends for i in range(pieces)], axis=0
        )
    high = matrix.astype(jnp.bfloat16)
    low = (matrix - high.astype(jnp.float32)).astype(jnp.bfloat16)
    both = jnp.concatenate([high, low], axis=1)
    return jnp.concatenate([both, both], axis=0)


def mix_lanes(values, both):
    high = values.astype(jnp.bfloat16)
    low = (values - high.astype(jnp.float32)).astype(jnp.bfloat16)
    out = jnp.dot(
        jnp.concatenate([high, low], axis=1), both, preferred_element_type=jnp.float32
    )
    return out[:, :SIDE] + out[:, SIDE:]


def own_place():
    return lax.axis_index("qa") * lax.axis_size("qb") + lax.axis_index("qb")


def bit_counts(place):
    row = lax.broadcasted_iota(jnp.int32, (SIDE, SIDE), 0)
    lane = lax.broadcasted_iota(jnp.int32, (SIDE, SIDE), 1)
    total = jnp.full((SIDE, SIDE), place, jnp.int32)
    count = jnp.zeros((SIDE, SIDE), jnp.int32)
    for bit in range(BITS):
        count = count + ((row >> bit) & 1) + ((lane >> bit) & 1) + ((total >> bit) & 1)
    return count


def every(step, first, count=SIDE):
    return pl.ds(first, count, stride=step)


def turned(real, imag, sine, cosine):
    return real * cosine + imag * sine, imag * cosine - real * sine


def mix_blocks(parts, pair):
    return [butterfly(part, [pair] * 2) for part in parts]


def in_buffer(buffer, out=None, step=TILE):
    def store(index, value, last):
        if value is None:
            return buffer[TILE * index : TILE * index + TILE, :]
        if last and out is not None:
            out[step * index : step * index + TILE, :] = value
        else:
            buffer[TILE * index : TILE * index + TILE, :] = value

    return store


def first_kernel(angles, diagonal, wave, levels, out, buffer):
    group = [pair_of(angles, 0, g) for g in range(4)]
    lane_mix = weights([group[0]] * BITS)
    count = bit_counts(own_place())
    speed = diagonal[0:1, :]
    real, imag = [], []
    for b in range(BLOCKS):
        level = levels[b]
        sine, cosine = sin_cos(level * speed, count + b.bit_count())
        r, i = turned(wave[0, b], wave[1, b], sine, cosine)
        real.append(r)
        imag.append(i)
        out[every(WIDE, TILE + b), :] = level
    for p, part in enumerate(mix_blocks((real, imag), group[2])):
        for b in range(BLOCKS):
            buffer[every(TILE, p * BLOCKS + b), :] = mix_lanes(part[b], lane_mix)
    store = in_buffer(buffer, out, WIDE)
    mix_tiles(lambda i: store(i, None, 0), store, [group[1]] * BITS)


def middle(layer, got, out, buffer, before, speed, lane_mix, next_mix, group, send_levels):
    store = in_buffer(buffer)
    mix_tiles(lambda i: got[WIDE * i : WIDE * i + TILE, :], store, before)
    step = WIDE if send_levels else TILE
    real, imag = [], []
    for b in range(BLOCKS):
        level = got[every(WIDE, TILE + b), :]
        sine, cosine = sin_cos(level * speed)
        r, i = turned(
            buffer[every(TILE, b), :], buffer[every(TILE, BLOCKS + b), :], sine, cosine
        )
        real.append(r)
        imag.append(i)
        if send_levels:
            out[every(step, TILE + b), :] = level.T
    for p, part in enumerate(mix_blocks((real, imag), group[2])):
        for b in range(BLOCKS):
            mixed = mix_lanes(mix_lanes(part[b], lane_mix).T, next_mix)
            out[every(step, p * BLOCKS + b), :] = mixed


def q_pairs(qa_pair, qb_pair):
    return [qb_pair] * QB_BITS + [qa_pair] * (BITS - QB_BITS)


def second_kernel(angles, diagonal, got, out, buffer):
    before = q_pairs(pair_of(angles, 0, 2), pair_of(angles, 0, 3))
    group = [pair_of(angles, 1, g) for g in range(4)]
    lane_mix = weights([group[0]] * BITS)
    q_mix = weights(q_pairs(group[2], group[3]))
    middle(1, got, out, buffer, before, diagonal[1:2, :], lane_mix, q_mix, group, True)


def third_kernel(angles, diagonal, got, out, buffer):
    group = [pair_of(angles, 2, g) for g in range(4)]
    q_mix = weights(q_pairs(group[2], group[3]))
    row_mix = weights([group[1]] * BITS)
    lane = lax.broadcasted_iota(jnp.int32, (1, SIDE), 1)
    own = jnp.where(lane == own_place(), diagonal[2:3, :], 0.0)
    speed = jnp.sum(own, axis=1, keepdims=True)
    before = [pair_of(angles, 1, 1)] * BITS
    middle(2, got, out, buffer, before, speed, q_mix, row_mix, group, False)


def last_kernel(angles, got, out_far, buffer, out, sems):
    store = in_buffer(buffer)
    mix_tiles(
        lambda i: got[TILE * i : TILE * i + TILE, :], store, [pair_of(angles, 2, 0)] * BITS
    )
    count = bit_counts(own_place())
    copies = []
    for b in range(BLOCKS):
        real, imag = (buffer[every(TILE, p * BLOCKS + b), :].T for p in range(PARTS))
        turns = count + b.bit_count()
        odd = (turns & 1) == 1
        new_real, new_imag = jnp.where(odd, -imag, real), jnp.where(odd, real, imag)
        back = (turns & 2) != 0
        out[0, b] = jnp.where(back, -new_real, new_real)
        out[1, b] = jnp.where(back, -new_imag, new_imag)
        for p in range(PARTS):
            copy = pltpu.make_async_copy(out.at[p, b], out_far.at[p, b], sems.at[p, b])
            copy.start()
            copies.append(copy)
    for copy in copies:
        copy.wait()


NEAR = pl.BlockSpec(memory_space=pltpu.VMEM)
FAR = pl.BlockSpec(memory_space=pl.ANY)
STATE = (PARTS, BLOCKS, SIDE, SIDE)


def call(kernel, name, operands, in_specs, out_shape, out_spec=NEAR, scratch=()):
    return pl.pallas_call(
        kernel,
        name=name,
        in_specs=in_specs,
        out_specs=out_spec,
        out_shape=jax.ShapeDtypeStruct(out_shape, jnp.float32),
        scratch_shapes=[pltpu.VMEM((SIDE * TILE, SIDE), jnp.float32), *scratch],
        compiler_params=pltpu.CompilerParams(vmem_limit_bytes=32 * 1024 * 1024),
        interpret=INTERPRET,
    )(*operands)


INTERPRET = False


def exchange(values):
    rows = values.shape[0] // SIDE
    shape = (SIDE, rows // 8, 8, SIDE) if rows % 8 == 0 else (SIDE, rows // 4, 4, SIDE)
    moved = lax.all_to_all(
        values.reshape(shape), ("qa", "qb"), split_axis=0, concat_axis=0, tiled=True
    )
    return moved.reshape(values.shape)


def shards(wave_parts, level_table, diagonal_angles, turn_angles):
    wide, narrow = (SIDE * WIDE, SIDE), (SIDE * TILE, SIDE)
    small = (turn_angles, diagonal_angles)
    values = call(
        first_kernel,
        "first",
        (*small, wave_parts, level_table),
        [NEAR] * 4,
        wide,
    )
    values = call(second_kernel, "second", (*small, exchange(values)), [NEAR] * 3, wide)
    values = call(third_kernel, "third", (*small, exchange(values)), [NEAR] * 3, narrow)
    return call(
        last_kernel,
        "last",
        (turn_angles, exchange(values)),
        [NEAR] * 2,
        STATE,
        FAR,
        scratch=[pltpu.VMEM(STATE, jnp.float32), pltpu.SemaphoreType.DMA((PARTS, BLOCKS))],
    )


def solution(mesh):
    placed = (
        P("trial", ("qa", "qb"), None, None),
        P(("trial", "qa", "qb"), None, None),
        P("trial", None),
        P("trial", None),
    )
    return jax.shard_map(
        shards,
        mesh=mesh,
        in_specs=placed,
        out_specs=P("trial", ("qa", "qb"), None, None),
        check_vma=False,
    )
```

```python
import jax
import jax.numpy as jnp
from jax import lax
from jax.experimental import pallas as pl
from jax.experimental.pallas import tpu as pltpu
from jax.sharding import PartitionSpec as P

SIDE = 128
LAYERS = 3
BITS = 7
BLOCKS = 4
PARTS = 2
TILE = PARTS * BLOCKS
WIDE = TILE + BLOCKS
QB_BITS = 3


def sin_cos(angle, turns=None):
    near = jnp.floor(angle * 0.6366197723675814 + 0.5)
    left = (angle - near * 1.5703125) - near * 4.8382679489661926e-4
    quarter = near.astype(jnp.int32)
    if turns is not None:
        quarter = quarter + turns
    sq = left * left
    sine = left + left * sq * (-1.6666654611e-1 + sq * (8.3321608736e-3 - sq * 1.9515295891e-4))
    cosine = (1.0 - 0.5 * sq) + sq * sq * (
        4.166664568298827e-2 + sq * (-1.388731625493765e-3 + sq * 2.443315711809948e-5)
    )
    odd = (quarter & 1) == 1
    new_sine = jnp.where(odd, cosine, sine)
    new_cosine = jnp.where(odd, sine, cosine)
    new_sine = jnp.where((quarter & 2) != 0, -new_sine, new_sine)
    new_cosine = jnp.where(((quarter + 1) & 2) != 0, -new_cosine, new_cosine)
    return new_sine, new_cosine


def pair_of(angles, layer, group):
    row = LAYERS + layer
    sine, cosine = sin_cos(jnp.broadcast_to(angles[row : row + 1, group : group + 1], (1, SIDE)))
    return sine, cosine, sine / cosine


def butterfly(values, pairs):
    values = list(values)
    for bit, (_, _, tangent) in enumerate(pairs):
        step = 1 << bit
        for low in range(len(values)):
            if not low & step:
                u, v = values[low], values[low + step]
                values[low] = u + tangent * v
                values[low + step] = v - tangent * u
    return values


def shrink(pairs):
    product = pairs[0][1]
    for pair in pairs[1:]:
        product = product * pair[1]
    return product


def mix_tiles(load, store, pairs):
    for high in range(0, SIDE, 8):
        for i, value in enumerate(butterfly([load(high + i) for i in range(8)], pairs[:3])):
            store(high + i, value, 0)
    for low in range(8):
        order = range(low, SIDE, 8)
        for i, value in zip(order, butterfly([store(i, None, 0) for i in order], pairs[3:])):
            store(i, value, 1)


def weights(pairs, scale=1.0):
    lane = lax.broadcasted_iota(jnp.int32, (8, SIDE), 1)
    sub = lax.broadcasted_iota(jnp.int32, (8, SIDE), 0)

    def factor(bit, of):
        to = (lane >> bit) & 1
        sine, cosine, _ = pairs[bit]
        return jnp.where(of == to, cosine, jnp.where(to == 1, -sine, sine))

    matrix = scale * factor(0, sub & 1) * factor(1, (sub >> 1) & 1) * factor(2, (sub >> 2) & 1)
    for bit in range(3, BITS):
        ends = [factor(bit, jnp.full((8, SIDE), of, jnp.int32)) for of in (0, 1)]
        pieces = matrix.shape[0] // 8
        matrix = jnp.concatenate(
            [matrix[8 * i : 8 * i + 8] * end for end in ends for i in range(pieces)], axis=0
        )
    high = matrix.astype(jnp.bfloat16)
    low = (matrix - high.astype(jnp.float32)).astype(jnp.bfloat16)
    both = jnp.concatenate([high, low], axis=1)
    return jnp.concatenate([both, both], axis=0)


def mix_lanes(values, both):
    high = values.astype(jnp.bfloat16)
    low = (values - high.astype(jnp.float32)).astype(jnp.bfloat16)
    out = jnp.dot(
        jnp.concatenate([high, low], axis=1), both, preferred_element_type=jnp.float32
    )
    return out[:, :SIDE] + out[:, SIDE:]


def own_place():
    return lax.axis_index("qa") * lax.axis_size("qb") + lax.axis_index("qb")


def bit_counts(place):
    row = lax.broadcasted_iota(jnp.int32, (SIDE, SIDE), 0)
    lane = lax.broadcasted_iota(jnp.int32, (SIDE, SIDE), 1)
    total = jnp.full((SIDE, SIDE), place, jnp.int32)
    count = jnp.zeros((SIDE, SIDE), jnp.int32)
    for bit in range(BITS):
        count = count + ((row >> bit) & 1) + ((lane >> bit) & 1) + ((total >> bit) & 1)
    return count


def every(step, first, count=SIDE):
    return pl.ds(first, count, stride=step)


def turned(real, imag, sine, cosine):
    return real * cosine + imag * sine, imag * cosine - real * sine


def mix_blocks(parts, pair):
    return [butterfly(part, [pair] * 2) for part in parts]


def in_buffer(buffer, out=None, step=TILE):
    def store(index, value, last):
        if value is None:
            return buffer[TILE * index : TILE * index + TILE, :]
        if last and out is not None:
            out[step * index : step * index + TILE, :] = value
        else:
            buffer[TILE * index : TILE * index + TILE, :] = value

    return store


def first_kernel(angles, wave, levels, out, buffer):
    group = [pair_of(angles, 0, g) for g in range(4)]
    after = [group[1]] * BITS
    lane_mix = weights([group[0]] * BITS, shrink(after + [group[2]] * 2))
    count = bit_counts(own_place())
    speed = angles[0:1, :]
    real, imag = [], []
    for b in range(BLOCKS):
        level = levels[b]
        sine, cosine = sin_cos(level * speed, count + b.bit_count())
        r, i = turned(wave[0, b], wave[1, b], sine, cosine)
        real.append(r)
        imag.append(i)
        out[every(WIDE, TILE + b), :] = level
    for p, part in enumerate(mix_blocks((real, imag), group[2])):
        for b in range(BLOCKS):
            buffer[every(TILE, p * BLOCKS + b), :] = mix_lanes(part[b], lane_mix)
    store = in_buffer(buffer, out, WIDE)
    mix_tiles(lambda i: store(i, None, 0), store, after)


def middle(layer, got, out, buffer, before, speed, lane_mix, next_mix, group, send_levels):
    store = in_buffer(buffer)
    mix_tiles(lambda i: got[WIDE * i : WIDE * i + TILE, :], store, before)
    step = WIDE if send_levels else TILE
    real, imag = [], []
    for b in range(BLOCKS):
        level = got[every(WIDE, TILE + b), :]
        sine, cosine = sin_cos(level * speed)
        r, i = turned(
            buffer[every(TILE, b), :], buffer[every(TILE, BLOCKS + b), :], sine, cosine
        )
        real.append(r)
        imag.append(i)
        if send_levels:
            out[every(step, TILE + b), :] = level.T
    for p, part in enumerate(mix_blocks((real, imag), group[2])):
        for b in range(BLOCKS):
            mixed = mix_lanes(mix_lanes(part[b], lane_mix).T, next_mix)
            out[every(step, p * BLOCKS + b), :] = mixed


def q_pairs(qa_pair, qb_pair):
    return [qb_pair] * QB_BITS + [qa_pair] * (BITS - QB_BITS)


def second_kernel(angles, got, out, buffer):
    before = q_pairs(pair_of(angles, 0, 2), pair_of(angles, 0, 3))
    group = [pair_of(angles, 1, g) for g in range(4)]
    lane_mix = weights([group[0]] * BITS, shrink(before + [group[2]] * 2))
    q_mix = weights(q_pairs(group[2], group[3]))
    middle(1, got, out, buffer, before, angles[1:2, :], lane_mix, q_mix, group, True)


def third_kernel(angles, got, out, buffer):
    group = [pair_of(angles, 2, g) for g in range(4)]
    before = [pair_of(angles, 1, 1)] * BITS
    q_mix = weights(q_pairs(group[2], group[3]), shrink(before + [group[2]] * 2))
    row_mix = weights([group[1]] * BITS, shrink([group[0]] * BITS))
    lane = lax.broadcasted_iota(jnp.int32, (1, SIDE), 1)
    own = jnp.where(lane == own_place(), angles[2:3, :], 0.0)
    speed = jnp.sum(own, axis=1, keepdims=True)
    middle(2, got, out, buffer, before, speed, q_mix, row_mix, group, False)


def last_kernel(angles, got, out_far, buffer, out, sems):
    store = in_buffer(buffer)
    mix_tiles(
        lambda i: got[TILE * i : TILE * i + TILE, :], store, [pair_of(angles, 2, 0)] * BITS
    )
    count = bit_counts(own_place())
    copies = []
    for b in range(BLOCKS):
        real, imag = (buffer[every(TILE, p * BLOCKS + b), :].T for p in range(PARTS))
        turns = count + b.bit_count()
        odd = (turns & 1) == 1
        new_real, new_imag = jnp.where(odd, -imag, real), jnp.where(odd, real, imag)
        back = (turns & 2) != 0
        out[0, b] = jnp.where(back, -new_real, new_real)
        out[1, b] = jnp.where(back, -new_imag, new_imag)
        for p in range(PARTS):
            copy = pltpu.make_async_copy(out.at[p, b], out_far.at[p, b], sems.at[p, b])
            copy.start()
            copies.append(copy)
    for copy in copies:
        copy.wait()


NEAR = pl.BlockSpec(memory_space=pltpu.VMEM)
FAR = pl.BlockSpec(memory_space=pl.ANY)
STATE = (PARTS, BLOCKS, SIDE, SIDE)


def call(kernel, name, operands, in_specs, out_shape, out_spec=NEAR, scratch=()):
    return pl.pallas_call(
        kernel,
        name=name,
        in_specs=in_specs,
        out_specs=out_spec,
        out_shape=jax.ShapeDtypeStruct(out_shape, jnp.float32),
        scratch_shapes=[pltpu.VMEM((SIDE * TILE, SIDE), jnp.float32), *scratch],
        compiler_params=pltpu.CompilerParams(vmem_limit_bytes=32 * 1024 * 1024),
        interpret=INTERPRET,
    )(*operands)


INTERPRET = False


def exchange(values):
    rows = values.shape[0] // SIDE
    shape = (SIDE, rows // 8, 8, SIDE) if rows % 8 == 0 else (SIDE, rows // 4, 4, SIDE)
    moved = lax.all_to_all(
        values.reshape(shape), ("qa", "qb"), split_axis=0, concat_axis=0, tiled=True
    )
    return moved.reshape(values.shape)


def shards(wave_parts, level_table, diagonal_angles, turn_angles):
    wide, narrow = (SIDE * WIDE, SIDE), (SIDE * TILE, SIDE)
    rest = SIDE - turn_angles.shape[1]
    angles = jnp.concatenate([diagonal_angles, jnp.pad(turn_angles, ((0, 0), (0, rest)))])
    values = call(
        first_kernel,
        "first",
        (angles, wave_parts, level_table),
        [NEAR] * 3,
        wide,
    )
    values = call(second_kernel, "second", (angles, exchange(values)), [NEAR] * 2, wide)
    values = call(third_kernel, "third", (angles, exchange(values)), [NEAR] * 2, narrow)
    return call(
        last_kernel,
        "last",
        (angles, exchange(values)),
        [NEAR] * 2,
        STATE,
        FAR,
        scratch=[pltpu.VMEM(STATE, jnp.float32), pltpu.SemaphoreType.DMA((PARTS, BLOCKS))],
    )


def solution(mesh):
    placed = (
        P("trial", ("qa", "qb"), None, None),
        P(("trial", "qa", "qb"), None, None),
        P("trial", None),
        P("trial", None),
    )
    return jax.shard_map(
        shards,
        mesh=mesh,
        in_specs=placed,
        out_specs=P("trial", ("qa", "qb"), None, None),
        check_vma=False,
    )
```

```python
import jax
import jax.numpy as jnp
from jax import lax
from jax.experimental import pallas as pl
from jax.experimental.pallas import tpu as pltpu
from jax.sharding import PartitionSpec as P

SIDE = 128
BITS = 7
BLOCKS = 4
PARTS = 2
TILE = PARTS * BLOCKS
WIDE = TILE + BLOCKS
QB_BITS = 3


def sin_cos(angle, turns=None):
    near = jnp.floor(angle * 0.6366197723675814 + 0.5)
    left = (angle - near * 1.5703125) - near * 4.8382679489661926e-4
    quarter = near.astype(jnp.int32)
    if turns is not None:
        quarter = quarter + turns
    sq = left * left
    sine = left + left * sq * (-1.6666654611e-1 + sq * (8.3321608736e-3 - sq * 1.9515295891e-4))
    cosine = (1.0 - 0.5 * sq) + sq * sq * (
        4.166664568298827e-2 + sq * (-1.388731625493765e-3 + sq * 2.443315711809948e-5)
    )
    odd = (quarter & 1) == 1
    new_sine = jnp.where(odd, cosine, sine)
    new_cosine = jnp.where(odd, sine, cosine)
    new_sine = jnp.where((quarter & 2) != 0, -new_sine, new_sine)
    new_cosine = jnp.where(((quarter + 1) & 2) != 0, -new_cosine, new_cosine)
    return new_sine, new_cosine


def pair_of(angles, layer, group):
    sine, cosine = sin_cos(jnp.broadcast_to(angles[layer : layer + 1, group : group + 1], (1, SIDE)))
    return sine, cosine, sine / cosine


def butterfly(values, pairs):
    values = list(values)
    for bit, (_, _, tangent) in enumerate(pairs):
        step = 1 << bit
        for low in range(len(values)):
            if not low & step:
                u, v = values[low], values[low + step]
                values[low] = u + tangent * v
                values[low + step] = v - tangent * u
    return values


def shrink(pairs):
    product = pairs[0][1]
    for pair in pairs[1:]:
        product = product * pair[1]
    return product


def mix_tiles(load, store, pairs):
    for high in range(0, SIDE, 8):
        for i, value in enumerate(butterfly([load(high + i) for i in range(8)], pairs[:3])):
            store(high + i, value, 0)
    for low in range(8):
        order = range(low, SIDE, 8)
        for i, value in zip(order, butterfly([store(i, None, 0) for i in order], pairs[3:])):
            store(i, value, 1)


def weights(pairs, scale=1.0):
    lane = lax.broadcasted_iota(jnp.int32, (8, SIDE), 1)
    sub = lax.broadcasted_iota(jnp.int32, (8, SIDE), 0)

    def factor(bit, of):
        to = (lane >> bit) & 1
        sine, cosine, _ = pairs[bit]
        return jnp.where(of == to, cosine, jnp.where(to == 1, -sine, sine))

    matrix = scale * factor(0, sub & 1) * factor(1, (sub >> 1) & 1) * factor(2, (sub >> 2) & 1)
    for bit in range(3, BITS):
        ends = [factor(bit, jnp.full((8, SIDE), of, jnp.int32)) for of in (0, 1)]
        pieces = matrix.shape[0] // 8
        matrix = jnp.concatenate(
            [matrix[8 * i : 8 * i + 8] * end for end in ends for i in range(pieces)], axis=0
        )
    high = matrix.astype(jnp.bfloat16)
    low = (matrix - high.astype(jnp.float32)).astype(jnp.bfloat16)
    both = jnp.concatenate([high, low], axis=1)
    return jnp.concatenate([both, both], axis=0)


def mix_lanes(values, both):
    high = values.astype(jnp.bfloat16)
    low = (values - high.astype(jnp.float32)).astype(jnp.bfloat16)
    out = jnp.dot(
        jnp.concatenate([high, low], axis=1), both, preferred_element_type=jnp.float32
    )
    return out[:, :SIDE] + out[:, SIDE:]


def own_place():
    return lax.axis_index("qa") * lax.axis_size("qb") + lax.axis_index("qb")


def bit_counts(place):
    row = lax.broadcasted_iota(jnp.int32, (SIDE, SIDE), 0)
    lane = lax.broadcasted_iota(jnp.int32, (SIDE, SIDE), 1)
    total = jnp.full((SIDE, SIDE), place, jnp.int32)
    count = jnp.zeros((SIDE, SIDE), jnp.int32)
    for bit in range(BITS):
        count = count + ((row >> bit) & 1) + ((lane >> bit) & 1) + ((total >> bit) & 1)
    return count


def every(step, first, count=SIDE):
    return pl.ds(first, count, stride=step)


def turned(real, imag, sine, cosine):
    return real * cosine + imag * sine, imag * cosine - real * sine


def mix_blocks(parts, pair):
    return [butterfly(part, [pair] * 2) for part in parts]


def in_buffer(buffer, out=None, step=TILE):
    def store(index, value, last):
        if value is None:
            return buffer[TILE * index : TILE * index + TILE, :]
        if last and out is not None:
            out[step * index : step * index + TILE, :] = value
        else:
            buffer[TILE * index : TILE * index + TILE, :] = value

    return store


def first_kernel(
    angles_far, diagonal_far, wave_far, levels_far, out, buffer, angles, diagonal, wave, levels, sems
):
    def copies(b):
        return [
            pltpu.make_async_copy(levels_far.at[b], levels.at[b], sems.at[0, b]),
            pltpu.make_async_copy(wave_far.at[0, b], wave.at[0, b], sems.at[1, b]),
            pltpu.make_async_copy(wave_far.at[1, b], wave.at[1, b], sems.at[2, b]),
        ]

    small = [
        pltpu.make_async_copy(angles_far, angles, sems.at[3, 0]),
        pltpu.make_async_copy(diagonal_far, diagonal, sems.at[3, 1]),
    ]
    for copy in small:
        copy.start()
    for b in range(BLOCKS):
        for copy in copies(b):
            copy.start()
    for copy in small:
        copy.wait()
    group = [pair_of(angles, 0, g) for g in range(4)]
    after = [group[1]] * BITS
    lane_mix = weights([group[0]] * BITS, shrink(after + [group[2]] * 2))
    count = bit_counts(own_place())
    speed = diagonal[0:1, :]
    real, imag = [], []
    for b in range(BLOCKS):
        for copy in copies(b):
            copy.wait()
        level = levels[b]
        sine, cosine = sin_cos(level * speed, count + b.bit_count())
        r, i = turned(wave[0, b], wave[1, b], sine, cosine)
        real.append(r)
        imag.append(i)
        out[every(WIDE, TILE + b), :] = level
    for p, part in enumerate(mix_blocks((real, imag), group[2])):
        for b in range(BLOCKS):
            buffer[every(TILE, p * BLOCKS + b), :] = mix_lanes(part[b], lane_mix)
    store = in_buffer(buffer, out, WIDE)
    mix_tiles(lambda i: store(i, None, 0), store, after)


def middle(layer, got, out, buffer, before, speed, lane_mix, next_mix, group, send_levels):
    store = in_buffer(buffer)
    mix_tiles(lambda i: got[WIDE * i : WIDE * i + TILE, :], store, before)
    step = WIDE if send_levels else TILE
    real, imag = [], []
    for b in range(BLOCKS):
        level = got[every(WIDE, TILE + b), :]
        sine, cosine = sin_cos(level * speed)
        r, i = turned(
            buffer[every(TILE, b), :], buffer[every(TILE, BLOCKS + b), :], sine, cosine
        )
        real.append(r)
        imag.append(i)
        if send_levels:
            out[every(step, TILE + b), :] = level.T
    for p, part in enumerate(mix_blocks((real, imag), group[2])):
        for b in range(BLOCKS):
            mixed = mix_lanes(mix_lanes(part[b], lane_mix).T, next_mix)
            out[every(step, p * BLOCKS + b), :] = mixed


def q_pairs(qa_pair, qb_pair):
    return [qb_pair] * QB_BITS + [qa_pair] * (BITS - QB_BITS)


def second_kernel(angles, diagonal, got, out, buffer):
    before = q_pairs(pair_of(angles, 0, 2), pair_of(angles, 0, 3))
    group = [pair_of(angles, 1, g) for g in range(4)]
    lane_mix = weights([group[0]] * BITS, shrink(before + [group[2]] * 2))
    q_mix = weights(q_pairs(group[2], group[3]))
    middle(1, got, out, buffer, before, diagonal[1:2, :], lane_mix, q_mix, group, True)


def third_kernel(angles, diagonal, got, out, buffer):
    group = [pair_of(angles, 2, g) for g in range(4)]
    before = [pair_of(angles, 1, 1)] * BITS
    q_mix = weights(q_pairs(group[2], group[3]), shrink(before + [group[2]] * 2))
    row_mix = weights([group[1]] * BITS, shrink([group[0]] * BITS))
    lane = lax.broadcasted_iota(jnp.int32, (1, SIDE), 1)
    own = jnp.where(lane == own_place(), diagonal[2:3, :], 0.0)
    speed = jnp.sum(own, axis=1, keepdims=True)
    middle(2, got, out, buffer, before, speed, q_mix, row_mix, group, False)


def last_kernel(angles, got, out_far, buffer, out, sems):
    store = in_buffer(buffer)
    mix_tiles(
        lambda i: got[TILE * i : TILE * i + TILE, :], store, [pair_of(angles, 2, 0)] * BITS
    )
    count = bit_counts(own_place())
    copies = []
    for b in range(BLOCKS):
        real, imag = (buffer[every(TILE, p * BLOCKS + b), :].T for p in range(PARTS))
        turns = count + b.bit_count()
        odd = (turns & 1) == 1
        new_real, new_imag = jnp.where(odd, -imag, real), jnp.where(odd, real, imag)
        back = (turns & 2) != 0
        out[0, b] = jnp.where(back, -new_real, new_real)
        out[1, b] = jnp.where(back, -new_imag, new_imag)
        for p in range(PARTS):
            copy = pltpu.make_async_copy(out.at[p, b], out_far.at[p, b], sems.at[p, b])
            copy.start()
            copies.append(copy)
    for copy in copies:
        copy.wait()


NEAR = pl.BlockSpec(memory_space=pltpu.VMEM)
FAR = pl.BlockSpec(memory_space=pl.ANY)
STATE = (PARTS, BLOCKS, SIDE, SIDE)


def call(kernel, name, operands, in_specs, out_shape, out_spec=NEAR, scratch=(), grant=32 << 20):
    return pl.pallas_call(
        kernel,
        name=name,
        in_specs=in_specs,
        out_specs=out_spec,
        out_shape=jax.ShapeDtypeStruct(out_shape, jnp.float32),
        scratch_shapes=[pltpu.VMEM((SIDE * TILE, SIDE), jnp.float32), *scratch],
        compiler_params=pltpu.CompilerParams(vmem_limit_bytes=grant),
        interpret=INTERPRET,
    )(*operands)


INTERPRET = False


def exchange(values):
    rows = values.shape[0] // SIDE
    shape = (SIDE, rows // 8, 8, SIDE) if rows % 8 == 0 else (SIDE, rows // 4, 4, SIDE)
    moved = lax.all_to_all(
        values.reshape(shape), ("qa", "qb"), split_axis=0, concat_axis=0, tiled=True
    )
    return moved.reshape(values.shape)


def shards(wave_parts, level_table, diagonal_angles, turn_angles):
    wide, narrow = (SIDE * WIDE, SIDE), (SIDE * TILE, SIDE)
    angles, small = turn_angles, (turn_angles, diagonal_angles)
    values = call(
        first_kernel,
        "first",
        (*small, wave_parts, level_table),
        [FAR] * 4,
        wide,
        scratch=[
            pltpu.VMEM(turn_angles.shape, jnp.float32),
            pltpu.VMEM(diagonal_angles.shape, jnp.float32),
            pltpu.VMEM(STATE, jnp.float32),
            pltpu.VMEM(STATE[1:], jnp.float32),
            pltpu.SemaphoreType.DMA((4, BLOCKS)),
        ],
        grant=56 << 20,
    )
    values = call(second_kernel, "second", (*small, exchange(values)), [NEAR] * 3, wide)
    values = call(third_kernel, "third", (*small, exchange(values)), [NEAR] * 3, narrow)
    return call(
        last_kernel,
        "last",
        (angles, exchange(values)),
        [NEAR] * 2,
        STATE,
        FAR,
        scratch=[pltpu.VMEM(STATE, jnp.float32), pltpu.SemaphoreType.DMA((PARTS, BLOCKS))],
    )


def solution(mesh):
    placed = (
        P("trial", ("qa", "qb"), None, None),
        P(("trial", "qa", "qb"), None, None),
        P("trial", None),
        P("trial", None),
    )
    return jax.shard_map(
        shards,
        mesh=mesh,
        in_specs=placed,
        out_specs=P("trial", ("qa", "qb"), None, None),
        check_vma=False,
    )
```

```python
import jax
import jax.numpy as jnp
from jax import lax
from jax.experimental import pallas as pl
from jax.experimental.pallas import tpu as pltpu
from jax.sharding import PartitionSpec as P

SIDE = 128
BITS = 7
BLOCKS = 4
PARTS = 2
TILE = PARTS * BLOCKS
WIDE = TILE + BLOCKS
QB_BITS = 3


def sin_cos(angle, turns=None):
    near = jnp.floor(angle * 0.6366197723675814 + 0.5)
    left = (angle - near * 1.5703125) - near * 4.8382679489661926e-4
    quarter = near.astype(jnp.int32)
    if turns is not None:
        quarter = quarter + turns
    sq = left * left
    sine = left + left * sq * (-1.6666654611e-1 + sq * (8.3321608736e-3 - sq * 1.9515295891e-4))
    cosine = (1.0 - 0.5 * sq) + sq * sq * (
        4.166664568298827e-2 + sq * (-1.388731625493765e-3 + sq * 2.443315711809948e-5)
    )
    odd = (quarter & 1) == 1
    new_sine = jnp.where(odd, cosine, sine)
    new_cosine = jnp.where(odd, sine, cosine)
    new_sine = jnp.where((quarter & 2) != 0, -new_sine, new_sine)
    new_cosine = jnp.where(((quarter + 1) & 2) != 0, -new_cosine, new_cosine)
    return new_sine, new_cosine


def pair_of(angles, layer, group):
    sine, cosine = sin_cos(jnp.broadcast_to(angles[layer : layer + 1, group : group + 1], (1, SIDE)))
    return sine, cosine, sine / cosine


def butterfly(values, pairs):
    values = list(values)
    for bit, (_, _, tangent) in enumerate(pairs):
        step = 1 << bit
        for low in range(len(values)):
            if not low & step:
                u, v = values[low], values[low + step]
                values[low] = u + tangent * v
                values[low + step] = v - tangent * u
    return values


def shrink(pairs):
    product = pairs[0][1]
    for pair in pairs[1:]:
        product = product * pair[1]
    return product


def mix_tiles(load, store, pairs, done=lambda end: None):
    for low in range(8):
        order = range(low, SIDE, 8)
        for i, value in zip(order, butterfly([load(i) for i in order], pairs[3:])):
            store(i, value, 0)
    for high in range(0, SIDE, 8):
        values = [store(high + i, None, 0) for i in range(8)]
        for i, value in enumerate(butterfly(values, pairs[:3])):
            store(high + i, value, 1)
        done(high + 8)


def weights(pairs, scale=1.0):
    lane = lax.broadcasted_iota(jnp.int32, (8, SIDE), 1)
    sub = lax.broadcasted_iota(jnp.int32, (8, SIDE), 0)

    def factor(bit, of):
        to = (lane >> bit) & 1
        sine, cosine, _ = pairs[bit]
        return jnp.where(of == to, cosine, jnp.where(to == 1, -sine, sine))

    matrix = scale * factor(0, sub & 1) * factor(1, (sub >> 1) & 1) * factor(2, (sub >> 2) & 1)
    for bit in range(3, BITS):
        ends = [factor(bit, jnp.full((8, SIDE), of, jnp.int32)) for of in (0, 1)]
        pieces = matrix.shape[0] // 8
        matrix = jnp.concatenate(
            [matrix[8 * i : 8 * i + 8] * end for end in ends for i in range(pieces)], axis=0
        )
    high = matrix.astype(jnp.bfloat16)
    low = (matrix - high.astype(jnp.float32)).astype(jnp.bfloat16)
    both = jnp.concatenate([high, low], axis=1)
    return jnp.concatenate([both, both], axis=0)


def mix_lanes(values, both):
    high = values.astype(jnp.bfloat16)
    low = (values - high.astype(jnp.float32)).astype(jnp.bfloat16)
    out = jnp.dot(
        jnp.concatenate([high, low], axis=1), both, preferred_element_type=jnp.float32
    )
    return out[:, :SIDE] + out[:, SIDE:]


def own_place():
    return lax.axis_index("qa") * lax.axis_size("qb") + lax.axis_index("qb")


def bit_counts(place):
    row = lax.broadcasted_iota(jnp.int32, (SIDE, SIDE), 0)
    lane = lax.broadcasted_iota(jnp.int32, (SIDE, SIDE), 1)
    total = jnp.full((SIDE, SIDE), place, jnp.int32)
    count = jnp.zeros((SIDE, SIDE), jnp.int32)
    for bit in range(BITS):
        count = count + ((row >> bit) & 1) + ((lane >> bit) & 1) + ((total >> bit) & 1)
    return count


def every(step, first, count=SIDE):
    return pl.ds(first, count, stride=step)


def turned(real, imag, sine, cosine):
    return real * cosine + imag * sine, imag * cosine - real * sine


def mix_blocks(parts, pair):
    return [butterfly(part, [pair] * 2) for part in parts]


def in_buffer(buffer, out=None, step=TILE):
    def store(index, value, last):
        if value is None:
            return buffer[TILE * index : TILE * index + TILE, :]
        if last and out is not None:
            out[step * index : step * index + TILE, :] = value
        else:
            buffer[TILE * index : TILE * index + TILE, :] = value

    return store


def first_kernel(
    angles_far, diagonal_far, wave_far, levels_far, out_far, buffer, angles, diagonal, wave, levels, out, sems
):
    def copies(b):
        return [
            pltpu.make_async_copy(levels_far.at[b], levels.at[b], sems.at[0, b]),
            pltpu.make_async_copy(wave_far.at[0, b], wave.at[0, b], sems.at[1, b]),
            pltpu.make_async_copy(wave_far.at[1, b], wave.at[1, b], sems.at[2, b]),
        ]

    small = [
        pltpu.make_async_copy(angles_far, angles, sems.at[3, 0]),
        pltpu.make_async_copy(diagonal_far, diagonal, sems.at[3, 1]),
    ]
    for copy in small:
        copy.start()
    for b in range(BLOCKS):
        for copy in copies(b):
            copy.start()
    for copy in small:
        copy.wait()
    group = [pair_of(angles, 0, g) for g in range(4)]
    after = [group[1]] * BITS
    lane_mix = weights([group[0]] * BITS, shrink(after + [group[2]] * 2))
    count = bit_counts(own_place())
    speed = diagonal[0:1, :]
    real, imag = [], []
    for b in range(BLOCKS):
        for copy in copies(b):
            copy.wait()
        level = levels[b]
        sine, cosine = sin_cos(level * speed, count + b.bit_count())
        r, i = turned(wave[0, b], wave[1, b], sine, cosine)
        real.append(r)
        imag.append(i)
        out[every(WIDE, TILE + b), :] = level
    for p, part in enumerate(mix_blocks((real, imag), group[2])):
        for b in range(BLOCKS):
            buffer[every(TILE, p * BLOCKS + b), :] = mix_lanes(part[b], lane_mix)
    store = in_buffer(buffer, out, WIDE)
    quarter, leaving = SIDE // 4, []

    def done(end):
        if end % quarter == 0:
            rows = pl.ds(WIDE * (end - quarter), WIDE * quarter)
            copy = pltpu.make_async_copy(out.at[rows], out_far.at[rows], sems.at[4, end // quarter - 1])
            copy.start()
            leaving.append(copy)

    mix_tiles(lambda i: store(i, None, 0), store, after, done)
    for copy in leaving:
        copy.wait()


def middle(layer, got, out, buffer, before, speed, lane_mix, next_mix, group, send_levels):
    store = in_buffer(buffer)
    mix_tiles(lambda i: got[WIDE * i : WIDE * i + TILE, :], store, before)
    step = WIDE if send_levels else TILE
    real, imag = [], []
    for b in range(BLOCKS):
        level = got[every(WIDE, TILE + b), :]
        sine, cosine = sin_cos(level * speed)
        r, i = turned(
            buffer[every(TILE, b), :], buffer[every(TILE, BLOCKS + b), :], sine, cosine
        )
        real.append(r)
        imag.append(i)
        if send_levels:
            out[every(step, TILE + b), :] = level.T
    for p, part in enumerate(mix_blocks((real, imag), group[2])):
        for b in range(BLOCKS):
            mixed = mix_lanes(mix_lanes(part[b], lane_mix).T, next_mix)
            out[every(step, p * BLOCKS + b), :] = mixed


def q_pairs(qa_pair, qb_pair):
    return [qb_pair] * QB_BITS + [qa_pair] * (BITS - QB_BITS)


def second_kernel(angles, diagonal, got, out, buffer):
    before = q_pairs(pair_of(angles, 0, 2), pair_of(angles, 0, 3))
    group = [pair_of(angles, 1, g) for g in range(4)]
    lane_mix = weights([group[0]] * BITS, shrink(before + [group[2]] * 2))
    q_mix = weights(q_pairs(group[2], group[3]))
    middle(1, got, out, buffer, before, diagonal[1:2, :], lane_mix, q_mix, group, True)


def third_kernel(angles, diagonal, got, out, buffer):
    group = [pair_of(angles, 2, g) for g in range(4)]
    before = [pair_of(angles, 1, 1)] * BITS
    q_mix = weights(q_pairs(group[2], group[3]), shrink(before + [group[2]] * 2))
    row_mix = weights([group[1]] * BITS, shrink([group[0]] * BITS))
    lane = lax.broadcasted_iota(jnp.int32, (1, SIDE), 1)
    own = jnp.where(lane == own_place(), diagonal[2:3, :], 0.0)
    speed = jnp.sum(own, axis=1, keepdims=True)
    middle(2, got, out, buffer, before, speed, q_mix, row_mix, group, False)


def last_kernel(angles, got, out_far, buffer, out, sems):
    store = in_buffer(buffer)
    mix_tiles(
        lambda i: got[TILE * i : TILE * i + TILE, :], store, [pair_of(angles, 2, 0)] * BITS
    )
    count = bit_counts(own_place())
    copies = []
    for b in range(BLOCKS):
        real, imag = (buffer[every(TILE, p * BLOCKS + b), :].T for p in range(PARTS))
        turns = count + b.bit_count()
        odd = (turns & 1) == 1
        new_real, new_imag = jnp.where(odd, -imag, real), jnp.where(odd, real, imag)
        back = (turns & 2) != 0
        out[0, b] = jnp.where(back, -new_real, new_real)
        out[1, b] = jnp.where(back, -new_imag, new_imag)
        for p in range(PARTS):
            copy = pltpu.make_async_copy(out.at[p, b], out_far.at[p, b], sems.at[p, b])
            copy.start()
            copies.append(copy)
    for copy in copies:
        copy.wait()


NEAR = pl.BlockSpec(memory_space=pltpu.VMEM)
FAR = pl.BlockSpec(memory_space=pl.ANY)
STATE = (PARTS, BLOCKS, SIDE, SIDE)


def call(kernel, name, operands, in_specs, out_shape, out_spec=NEAR, scratch=(), grant=32 << 20):
    return pl.pallas_call(
        kernel,
        name=name,
        in_specs=in_specs,
        out_specs=out_spec,
        out_shape=jax.ShapeDtypeStruct(out_shape, jnp.float32),
        scratch_shapes=[pltpu.VMEM((SIDE * TILE, SIDE), jnp.float32), *scratch],
        compiler_params=pltpu.CompilerParams(vmem_limit_bytes=grant),
        interpret=INTERPRET,
    )(*operands)


INTERPRET = False


def exchange(values):
    rows = values.shape[0] // SIDE
    shape = (SIDE, rows // 8, 8, SIDE) if rows % 8 == 0 else (SIDE, rows // 4, 4, SIDE)
    moved = lax.all_to_all(
        values.reshape(shape), ("qa", "qb"), split_axis=0, concat_axis=0, tiled=True
    )
    return moved.reshape(values.shape)


def shards(wave_parts, level_table, diagonal_angles, turn_angles):
    wide, narrow = (SIDE * WIDE, SIDE), (SIDE * TILE, SIDE)
    angles, small = turn_angles, (turn_angles, diagonal_angles)
    values = call(
        first_kernel,
        "first",
        (*small, wave_parts, level_table),
        [FAR] * 4,
        wide,
        FAR,
        scratch=[
            pltpu.VMEM(turn_angles.shape, jnp.float32),
            pltpu.VMEM(diagonal_angles.shape, jnp.float32),
            pltpu.VMEM(STATE, jnp.float32),
            pltpu.VMEM(STATE[1:], jnp.float32),
            pltpu.VMEM(wide, jnp.float32),
            pltpu.SemaphoreType.DMA((5, BLOCKS)),
        ],
        grant=56 << 20,
    )
    values = call(second_kernel, "second", (*small, exchange(values)), [NEAR] * 3, wide)
    values = call(third_kernel, "third", (*small, exchange(values)), [NEAR] * 3, narrow)
    return call(
        last_kernel,
        "last",
        (angles, exchange(values)),
        [NEAR] * 2,
        STATE,
        FAR,
        scratch=[pltpu.VMEM(STATE, jnp.float32), pltpu.SemaphoreType.DMA((PARTS, BLOCKS))],
    )


def solution(mesh):
    placed = (
        P("trial", ("qa", "qb"), None, None),
        P(("trial", "qa", "qb"), None, None),
        P("trial", None),
        P("trial", None),
    )
    return jax.shard_map(
        shards,
        mesh=mesh,
        in_specs=placed,
        out_specs=P("trial", ("qa", "qb"), None, None),
        check_vma=False,
    )
```
